32 devices in a mesh: blk: 8 (over z, x), col: 4 (over y, core).
Axes of the slice: x: 2, y: 2, z: 4, core: 2. Of those that a mesh axis runs over, the one named last changes fastest.
Arguments:
- momentum: float32 [2048, 29568], P('blk', 'col'), may hold values from -200 to 200
- grad: bfloat16 [2048, 29568], P('blk', 'col'), may hold values from -6 to 6
- q_basis: bfloat16 [1024, 29568], P('blk', 'col'), may hold values from -6 to 6
Outputs:
- momentum_new: float32 [2048, 29568], P('blk', 'col')
- update: bfloat16 [2048, 29568], P('blk', 'col')
- q_new: bfloat16 [1024, 29568], P('blk', 'col')
The draws below stay inside these ranges and needn't reach their ends.
All inputs are finite; a program needn't handle non-finite values.
Results may differ from the reference program's by a relative error of at most 0.022.
Values may be sent and summed in bfloat16 or wider, within the bound.
A program may use at most 128 MiB of HBM per device.

```python
import jax
import jax.numpy as jnp
from jax import lax

FF = 29568
RANK = 1024
D_MODEL = 2048
N_BLK = 8
N_COL = 4


def draw_momentum(key, part):
    keys = jax.random.split(jax.random.fold_in(key, 11), 3)
    base = jax.random.truncated_normal(keys[0], -6.0, 6.0, (D_MODEL, FF), jnp.float32)
    row_rise = 0.5 + jnp.arange(D_MODEL, dtype=jnp.float32) / (D_MODEL - 1)
    row_spread = jnp.exp(jax.random.uniform(keys[1], (D_MODEL, 1), jnp.float32, -1.1513, 1.1513))
    col_spread = jnp.exp(jax.random.uniform(keys[2], (1, FF), jnp.float32, -1.1513, 1.1513))
    field = base * row_rise[:, None] * row_spread * col_spread
    return jnp.clip(field, -200.0, 200.0)


def block_levels(key, extent, cuts, least, largest):
    def one(position, blocks):
        draws = jax.random.uniform(jax.random.fold_in(jax.random.fold_in(key, 6), position), (blocks,), jnp.float32, least / len(cuts), largest / len(cuts))
        return jnp.repeat(jnp.exp(draws), extent[position] // blocks).reshape((-1,) + (1,) * (len(extent) - position - 1))

    loudness = one(*cuts[0])
    for cut in cuts[1:]:
        loudness = loudness * one(*cut)
    return loudness


def scatter_about(own_key, extent, spread, most, pieces=(), kind=jnp.bfloat16):
    factor_of = block_levels(own_key, extent, pieces, -0.22, 0.18) if pieces else 1.0
    result = jax.random.normal(own_key, extent, jnp.float32) * spread * factor_of
    return jnp.minimum(jnp.maximum(result, -most), most).astype(kind)


def setup_inputs(seed: int = 0) -> dict:
    arg_keys = jax.random.split(jax.random.key(seed), 4)
    return {
        "momentum": draw_momentum(jax.random.fold_in(arg_keys[3], 71), 0),
        "grad": scatter_about(arg_keys[1], (D_MODEL, FF), 1.0, 6.0, ((0, 8), (1, 4))),
        "q_basis": scatter_about(arg_keys[2], (RANK, FF), 1.0, 6.0, ((0, 8), (1, 4))),
    }


decay_rest = 0.05
epsilon = 1e-06

def reference(momentum, grad, q_basis):
    rows_total = momentum.shape[0]
    feature_count = momentum.shape[1]
    rank_count = q_basis.shape[0]
    b_matrix = momentum + grad.astype(jnp.float32)
    b_half = b_matrix.astype(jnp.bfloat16)
    col_width = feature_count // N_COL

    def p_step(index, running):
        start = (index * col_width).astype(jnp.int32)
        b_slice = lax.dynamic_slice_in_dim(b_half, start, col_width, 1)
        q_slice = lax.dynamic_slice_in_dim(q_basis, start, col_width, 1)
        partial_value = lax.dot_general(b_slice, q_slice, (((1,), (1,)), ((), ())), preferred_element_type=jnp.float32)
        rounded = lax.optimization_barrier(partial_value.astype(jnp.bfloat16))
        return running + rounded.astype(jnp.float32)
    p_matrix = lax.fori_loop(0, N_COL, p_step, jnp.zeros((rows_total, rank_count), jnp.float32))
    p_scale = jnp.sqrt(lax.optimization_barrier(jnp.sum(p_matrix * p_matrix, axis=0)) / rows_total + epsilon)
    p_hat = (p_matrix / p_scale[None, :]).astype(jnp.bfloat16)
    row_height = rows_total // N_BLK

    def r_step(index, running):
        start = (index * row_height).astype(jnp.int32)
        p_slice = lax.dynamic_slice_in_dim(p_hat, start, row_height, 0)
        b_slice = lax.dynamic_slice_in_dim(b_half, start, row_height, 0)
        partial_value = lax.dot_general(p_slice, b_slice, (((0,), (0,)), ((), ())), preferred_element_type=jnp.float32)
        rounded = lax.optimization_barrier(partial_value.astype(jnp.bfloat16))
        return running + rounded.astype(jnp.float32)
    r_matrix = lax.fori_loop(0, N_BLK, r_step, jnp.zeros((rank_count, feature_count), jnp.float32))
    r_scale = jnp.sqrt(lax.optimization_barrier(jnp.sum(r_matrix * r_matrix, axis=1)) / feature_count + epsilon)
    q_new = (r_matrix / r_scale[:, None]).astype(jnp.bfloat16)
    weighted = (p_hat.astype(jnp.float32) * (decay_rest * r_scale / rows_total)[None, :]).astype(jnp.bfloat16)
    update_sum = jnp.dot(p_hat, q_new, preferred_element_type=jnp.float32)
    correction = jnp.dot(weighted, q_new, preferred_element_type=jnp.float32)
    update = (update_sum * (1.0 / jnp.sqrt(jnp.float32(rank_count)))).astype(jnp.bfloat16)
    return (b_matrix - correction, update, q_new)
```

```python
import functools

import jax
import jax.numpy as jnp
from jax import lax
from jax.experimental import pallas as pl
from jax.experimental.pallas import tpu as pltpu
from jax.sharding import PartitionSpec as P

MESH = pl.DeviceIdType.MESH
decay_rest = 0.05
epsilon = 1e-06
LANES = 128
PARAMS = functools.partial(pltpu.CompilerParams, has_side_effects=True, vmem_limit_bytes=60 * 1024 * 1024)


def greet(peers):
    barrier = pltpu.get_barrier_semaphore()
    for peer in peers:
        pl.semaphore_signal(barrier, inc=1, device_id=peer, device_id_type=MESH)
    pl.semaphore_wait(barrier, len(peers))


def remote(src, dst, send, recv, peer):
    return pltpu.make_async_remote_copy(
        src_ref=src, dst_ref=dst, send_sem=send, recv_sem=recv, device_id=peer, device_id_type=MESH
    )


def spread_kernel(n_out, n_in, b_ref, q_ref, bz_ref, qf_ref, b_own, q_own, own_sem, sb, rb, sq, rq, sf, rf):
    blk, col = lax.axis_index("blk"), lax.axis_index("col")
    me_o, me_i = blk // n_in, lax.rem(blk, n_in)
    outer = [lax.rem(me_o + k, n_out) for k in range(n_out)]
    width = bz_ref.shape[-1]
    wide = [pl.ds(pl.multiple_of(o * width, LANES), width) for o in outer]
    inner = [lax.rem(me_i + k, n_in) for k in range(n_in)]
    greet(
        [(outer[k] * n_in + me_i, col) for k in range(1, n_out)]
        + [(me_o * n_in + inner[j], col) for j in range(1, n_in)]
    )
    load_b = pltpu.make_async_copy(b_ref.at[:, wide[0]], b_own, own_sem.at[0])
    load_q = pltpu.make_async_copy(q_ref.at[:, wide[0]], q_own, own_sem.at[1])
    load_b.start()
    load_q.start()
    q_sends, b_sends, forwards = [], [], []
    for k in range(1, n_out):
        peer = (outer[k] * n_in + me_i, col)
        copy = remote(q_ref.at[:, wide[k]], qf_ref.at[me_o, me_i], sq.at[k], rq.at[k], peer)
        copy.start()
        q_sends.append(copy)
    for j in range(1, n_in):
        peer = (me_o * n_in + inner[j], col)
        copy = remote(q_ref.at[:, wide[0]], qf_ref.at[me_o, me_i], sf.at[j, 0], rf.at[j, 0], peer)
        copy.start()
        forwards.append(copy)
    for k in range(1, n_out):
        peer = (outer[k] * n_in + me_i, col)
        copy = remote(b_ref.at[:, wide[k]], bz_ref.at[me_o], sb.at[k], rb.at[k], peer)
        copy.start()
        b_sends.append(copy)
    load_b.wait()
    load_q.wait()
    store_b = pltpu.make_async_copy(b_own, bz_ref.at[me_o], own_sem.at[0])
    store_q = pltpu.make_async_copy(q_own, qf_ref.at[me_o, me_i], own_sem.at[1])
    store_b.start()
    store_q.start()
    for k in range(1, n_out):
        q_sends[k - 1].wait_recv()
        came_from = lax.rem(me_o + n_out - k, n_out)
        for j in range(1, n_in):
            peer = (me_o * n_in + inner[j], col)
            piece = qf_ref.at[came_from, me_i]
            copy = remote(piece, piece, sf.at[j, k], rf.at[j, k], peer)
            copy.start()
            forwards.append(copy)
    for copy in q_sends:
        copy.wait_send()
    for copy in b_sends + forwards:
        copy.wait()
    store_b.wait()
    store_q.wait()


def spread(n_out, n_in, b_half, q_basis):
    width = b_half.shape[1] // n_out
    b_part = (b_half.shape[0], width)
    q_part = (q_basis.shape[0], width)
    any_space = pl.BlockSpec(memory_space=pl.ANY)
    dma = pltpu.SemaphoreType.DMA
    return pl.pallas_call(
        functools.partial(spread_kernel, n_out, n_in),
        out_shape=(
            jax.ShapeDtypeStruct((n_out,) + b_part, b_half.dtype),
            jax.ShapeDtypeStruct((n_out, n_in) + q_part, q_basis.dtype),
        ),
        in_specs=[any_space] * 2,
        out_specs=(any_space, any_space),
        scratch_shapes=[
            pltpu.VMEM(b_part, b_half.dtype),
            pltpu.VMEM(q_part, q_basis.dtype),
            dma((2,)),
            dma((n_out,)),
            dma((n_out,)),
            dma((n_out,)),
            dma((n_out,)),
            dma((n_in, n_out)),
            dma((n_in, n_out)),
        ],
        compiler_params=PARAMS(collective_id=0),
        name="spread",
    )(b_half, q_basis)


def left_kernel(
    n_out, n_in, n_col, n_core, rows_total, pt_ref, out_ref,
    half, summed, got, squares, squares_got, mine, s0, r0, s1, r1, s2, r2, s3, r3, s4, r4, own_sem
):
    blk, col = lax.axis_index("blk"), lax.axis_index("col")
    me_o, me_i = blk // n_in, lax.rem(blk, n_in)
    n_chip = n_col // n_core
    chip, core = col // n_core, lax.rem(col, n_core)
    members = n_out * n_chip
    me = me_o * n_chip + chip
    place, peers, source = [], [], []
    for k in range(members):
        g = lax.rem(me + k, members)
        place.append(g)
        peers.append(((g // n_chip) * n_in + me_i, lax.rem(g, n_chip) * n_core + core))
        source.append(lax.rem(me + members - k, members))
    inner_peers = [(me_o * n_in + lax.rem(me_i + j, n_in), col) for j in range(n_in)]
    cores = [lax.rem(core + j, n_core) for j in range(n_core)]
    core_peers = [(blk, chip * n_core + cores[j]) for j in range(n_core)]
    greet(peers[1:] + inner_peers[1:] + core_peers[1:])
    hand = []
    for j in range(1, n_core):
        copy = remote(pt_ref.at[cores[j]], half.at[j], s0.at[j], r0.at[j], core_peers[j])
        copy.start()
        hand.append(copy)
    for copy in hand:
        copy.wait_recv()

    def add_cores(g):
        total = pt_ref[core, g].astype(jnp.float32)
        for j in range(1, n_core):
            total = total + half[j, g].astype(jnp.float32)
        return total

    sends = []
    for k in list(range(1, members)) + [0]:
        summed[place[k]] = add_cores(place[k]).astype(summed.dtype)
        if k:
            copy = remote(summed.at[place[k]], got.at[k], s1.at[k], r1.at[k], peers[k])
            copy.start()
            sends.append(copy)
    total = add_cores(me)
    for k in range(1, members):
        sends[k - 1].wait_recv()
        total = total + got[k].astype(jnp.float32)
    square = jnp.sum(total * total, axis=1, keepdims=True)
    squares[...] = jnp.broadcast_to(square, squares.shape)
    swaps = []
    for j in range(1, n_in):
        copy = remote(squares, squares_got.at[j], s2.at[j], r2.at[j], inner_peers[j])
        copy.start()
        swaps.append(copy)
    full = squares[...]
    for j in range(1, n_in):
        swaps[j - 1].wait_recv()
        full = full + squares_got[j]
    scale = jnp.sqrt(full[:, :1] / rows_total + epsilon)
    mine[...] = (total / scale).astype(mine.dtype)
    own = pltpu.make_async_copy(mine, out_ref.at[core, me], own_sem.at[0])
    own.start()
    gathers, passes = [], []
    for k in range(1, members):
        copy = remote(mine, out_ref.at[core, me], s3.at[k], r3.at[k], peers[k])
        copy.start()
        gathers.append(copy)
    for j in range(1, n_core):
        copy = remote(mine, out_ref.at[core, me], s4.at[j, 0], r4.at[j, 0], core_peers[j])
        copy.start()
        passes.append(copy)
    for k in range(1, members):
        gathers[k - 1].wait_recv()
        for j in range(1, n_core):
            piece = out_ref.at[core, source[k]]
            copy = remote(piece, piece, s4.at[j, k], r4.at[j, k], core_peers[j])
            copy.start()
            passes.append(copy)
    for copy in hand + sends + swaps + gathers:
        copy.wait_send()
    for copy in passes:
        copy.wait()
    own.wait()


def left(n_out, n_in, n_col, rows_total, pt):
    n_core = 2 if n_col % 2 == 0 else 1
    members = n_out * n_col // n_core
    rank, rows = pt.shape
    part = rank // (members * n_core)
    dma = pltpu.SemaphoreType.DMA
    vmem = pl.BlockSpec(memory_space=pltpu.VMEM)
    shape = (n_core, members, part, rows)
    out = pl.pallas_call(
        functools.partial(left_kernel, n_out, n_in, n_col, n_core, rows_total),
        out_shape=jax.ShapeDtypeStruct(shape, pt.dtype),
        in_specs=[vmem],
        out_specs=vmem,
        scratch_shapes=[
            pltpu.VMEM(shape, pt.dtype),
            pltpu.VMEM((members, part, rows), pt.dtype),
            pltpu.VMEM((members, part, rows), pt.dtype),
            pltpu.VMEM((part, LANES), jnp.float32),
            pltpu.VMEM((n_in, part, LANES), jnp.float32),
            pltpu.VMEM((part, rows), pt.dtype),
        ]
        + [dma((n_core,))] * 2
        + [dma((members,))] * 2
        + [dma((n_in,))] * 2
        + [dma((members,))] * 2
        + [dma((n_core, members))] * 2
        + [dma((1,))],
        compiler_params=PARAMS(collective_id=1),
        name="left",
    )(pt.reshape(shape))
    return out.reshape(rank, rows)


def right_kernel(
    n_out, n_in, n_col, r_ref, full_ref, sum_ref,
    got, mine, squares, squares_got, s1, r1, sz, rz, sx, rx, s2, r2, s3, r3, own_sem
):
    blk, col = lax.axis_index("blk"), lax.axis_index("col")
    me_o, me_i = blk // n_in, lax.rem(blk, n_in)
    width = r_ref.shape[-1]
    inner = [lax.rem(me_i + j, n_in) for j in range(n_in)]
    origin = [lax.rem(me_i + n_in - j, n_in) for j in range(n_in)]
    peers = [(me_o * n_in + inner[j], col) for j in range(n_in)]
    members = n_out * n_col
    mates = []
    for k in range(members):
        g = lax.rem(me_o * n_col + col + k, members)
        mates.append(((g // n_col) * n_in + me_i, lax.rem(g, n_col)))
    greet(peers[1:] + mates[1:])
    first = list(range(n_out // 2))

    def slot(p, i, o):
        return full_ref.at[p, i, :, pl.ds(pl.multiple_of(o * width, LANES), width)]

    def along(way, s, p, d, source, piece):
        peer = ((me_o + 1 if way == 0 else me_o - 1) * n_in + me_i, col)
        return remote(source, piece, sz.at[way, s, p, d], rz.at[way, s, p, d], peer)

    def can_send(way):
        return me_o < n_out - 1 if way == 0 else me_o > 0

    def came(way, d):
        return (me_o - d, me_o >= d) if way == 0 else (me_o + d, me_o + d < n_out)

    def across(j, p, index, source, piece):
        return remote(source, piece, sx.at[j, p, index], rx.at[j, p, index], peers[j])

    def mark(way, d):
        return d if way == 0 else n_out - 1 + d

    sends = {}
    for p in range(n_out):
        for j in range(1, n_in):
            copy = remote(r_ref.at[p, inner[j]], got.at[j, p], s1.at[j, p], r1.at[j, p], peers[j])
            copy.start()
            sends[j, p] = copy
    squares[...] = jnp.zeros_like(squares)
    ones = jnp.ones((8, width), jnp.float32)
    for p in range(n_out):
        for j in range(1, n_in):
            sends[j, p].wait_recv()
        total = r_ref[p, me_i].astype(jnp.float32)
        for j in range(1, n_in):
            total = total + got[j, p].astype(jnp.float32)
        mine[p] = total.astype(mine.dtype)
        squares[p] = lax.dot_general(
            ones, total * total, (((1,), (1,)), ((), ())),
            precision=lax.Precision.HIGHEST, preferred_element_type=jnp.float32,
        )
        own = slot(p, me_i, me_o)
        pltpu.make_async_copy(mine.at[p], own, own_sem.at[p]).start()
        for j in range(1, n_in):
            across(j, p, 0, mine.at[p], own).start()
        for way in range(2):
            @pl.when(can_send(way))
            def _():
                along(way, 0, p, 1, mine.at[p], own).start()
    pooled = []
    for k in range(1, members):
        copy = remote(squares, squares_got.at[k], s2.at[k], r2.at[k], mates[k])
        copy.start()
        pooled.append(copy)
    for p in first:
        for j in range(1, n_in):
            piece = slot(p, origin[j], me_o)
            across(j, p, 0, piece, piece).wait_recv()
            for way in range(2):
                @pl.when(can_send(way))
                def _():
                    along(way, j, p, 1, piece, piece).start()
    for d in range(1, n_out):
        for p in list(range(len(first), n_out)) + first:
            for s in range(n_in if p in first else 1):
                for way in range(2):
                    o, there = came(way, d)

                    @pl.when(there)
                    def _():
                        piece = slot(p, origin[s], o)
                        along(way, s, p, d, piece, piece).wait_recv()
                        if d < n_out - 1:
                            @pl.when(can_send(way))
                            def _():
                                along(way, s, p, d + 1, piece, piece).start()
                        if p not in first:
                            for j in range(1, n_in):
                                across(j, p, mark(way, d), piece, piece).start()
    total = squares[...]
    for k in range(1, members):
        pooled[k - 1].wait_recv()
        total = total + squares_got[k]
    sum_ref[0] = total
    swaps = []
    for j in range(1, n_in):
        copy = remote(sum_ref.at[0], sum_ref.at[j], s3.at[j], r3.at[j], peers[j])
        copy.start()
        swaps.append(copy)
    for p in range(n_out):
        own = slot(p, me_i, me_o)
        pltpu.make_async_copy(mine.at[p], own, own_sem.at[p]).wait()
        for j in range(1, n_in):
            across(j, p, 0, mine.at[p], own).wait_send()
            if p not in first:
                piece = slot(p, origin[j], me_o)
                across(j, p, 0, piece, piece).wait_recv()
        for s in range(n_in if p in first else 1):
            for way in range(2):
                for d in range(1, n_out):
                    o, there = came(way, d - 1)

                    @pl.when(there & can_send(way))
                    def _():
                        piece = slot(p, origin[s], o)
                        along(way, s, p, d, piece, piece).wait_send()
        if p not in first:
            for way in range(2):
                for d in range(1, n_out):
                    o, there = came(way, d)

                    @pl.when(there)
                    def _():
                        for j in range(1, n_in):
                            mark_at = mark(way, d)
                            piece = slot(p, me_i, o)
                            across(j, p, mark_at, piece, piece).wait_send()
                            piece = slot(p, origin[j], o)
                            across(j, p, mark_at, piece, piece).wait_recv()
    for copy in list(sends.values()) + pooled:
        copy.wait_send()
    for copy in swaps:
        copy.wait()


def right(n_out, n_in, n_col, r):
    rank, width = r.shape
    part = rank // (n_out * n_in)
    members = n_out * n_col
    dma = pltpu.SemaphoreType.DMA
    vmem = pl.BlockSpec(memory_space=pltpu.VMEM)
    full, sums = pl.pallas_call(
        functools.partial(right_kernel, n_out, n_in, n_col),
        out_shape=(
            jax.ShapeDtypeStruct((n_out, n_in, part, n_out * width), r.dtype),
            jax.ShapeDtypeStruct((n_in, n_out, 8, part), jnp.float32),
        ),
        in_specs=[vmem],
        out_specs=(pl.BlockSpec(memory_space=pl.ANY), vmem),
        scratch_shapes=[
            pltpu.VMEM((n_in, n_out, part, width), r.dtype),
            pltpu.VMEM((n_out, part, width), r.dtype),
            pltpu.VMEM((n_out, 8, part), jnp.float32),
            pltpu.VMEM((members, n_out, 8, part), jnp.float32),
        ]
        + [dma((n_in, n_out))] * 2
        + [dma((2, n_in, n_out, n_out))] * 2
        + [dma((n_in, n_out, 2 * n_out - 1))] * 2
        + [dma((members,))] * 2
        + [dma((n_in,))] * 2
        + [dma((n_out,))],
        compiler_params=PARAMS(collective_id=2),
        name="right",
    )(r.reshape(n_out, n_in, part, width))
    me_i = lax.rem(lax.axis_index("blk"), n_in)
    order = lax.rem(me_i - jnp.arange(n_in) + n_in, n_in)
    sums = jnp.take(sums[:, :, 0, :], order, axis=0).transpose(1, 0, 2).reshape(rank)
    return full.reshape(rank, n_out * width), sums


def shards(n_blk, n_col, momentum, grad, q_basis):
    n_out = 4 if n_blk % 4 == 0 else n_blk
    n_in = n_blk // n_out
    rows, cols = momentum.shape
    rank_rows = q_basis.shape[0]
    rank = rank_rows * n_blk
    rows_total, feature_count = rows * n_blk, cols * n_col
    width = -(-cols // (n_out * LANES)) * LANES
    pad = ((0, 0), (0, n_out * width - cols))

    b_matrix = momentum + grad.astype(jnp.float32)
    bz, qf = spread(n_out, n_in, jnp.pad(b_matrix.astype(jnp.bfloat16), pad), jnp.pad(q_basis, pad))
    bz = bz.reshape(n_out * rows, width)
    qf = qf.reshape(rank, width)
    pt = lax.dot_general(qf, bz, (((1,), (1,)), ((), ())), preferred_element_type=jnp.float32)
    p_hat_t = left(n_out, n_in, n_col, rows_total, pt.astype(jnp.bfloat16))
    r_part = jnp.dot(p_hat_t, bz, preferred_element_type=jnp.float32).astype(jnp.bfloat16)
    r_sum, squares = right(n_out, n_in, n_col, r_part)
    r_scale = jnp.sqrt(squares / feature_count + epsilon)
    blk = lax.axis_index("blk")
    p_mine = lax.dynamic_slice_in_dim(p_hat_t, (blk // n_in) * rows, rows, 1)
    p_even = (p_mine.astype(jnp.float32) / r_scale[:, None]).astype(jnp.bfloat16)
    over = (((0,), (0,)), ((), ()))
    correction = lax.dot_general(p_mine, r_sum, over, preferred_element_type=jnp.float32)[:, :cols]
    update = lax.dot_general(p_even, r_sum, over, preferred_element_type=jnp.float32)[:, :cols]
    update = (update * (1.0 / jnp.sqrt(jnp.float32(rank)))).astype(jnp.bfloat16)
    start = blk * rank_rows
    r_mine = lax.dynamic_slice_in_dim(r_sum, start, rank_rows, 0)[:, :cols].astype(jnp.float32)
    scale_mine = lax.dynamic_slice_in_dim(r_scale, start, rank_rows, 0)
    q_new = (r_mine / scale_mine[:, None]).astype(jnp.bfloat16)
    return (b_matrix - correction * (decay_rest / rows_total), update, q_new)


def solution(mesh):
    in_specs = (P("blk", "col"), P("blk", "col"), P("blk", "col"))
    out_specs = (P("blk", "col"), P("blk", "col"), P("blk", "col"))
    body = functools.partial(shards, mesh.shape["blk"], mesh.shape["col"])
    return jax.shard_map(body, mesh=mesh, in_specs=in_specs, out_specs=out_specs, check_vma=False)
```

```python
import functools

import jax
import jax.numpy as jnp
from jax import lax
from jax.experimental import pallas as pl
from jax.experimental.pallas import tpu as pltpu
from jax.sharding import PartitionSpec as P

MESH = pl.DeviceIdType.MESH
decay_rest = 0.05
epsilon = 1e-06
LANES = 128
PARAMS = functools.partial(pltpu.CompilerParams, has_side_effects=True, vmem_limit_bytes=60 * 1024 * 1024)


def greet(peers):
    barrier = pltpu.get_barrier_semaphore()
    for peer in peers:
        pl.semaphore_signal(barrier, inc=1, device_id=peer, device_id_type=MESH)
    pl.semaphore_wait(barrier, len(peers))


def remote(src, dst, send, recv, peer):
    return pltpu.make_async_remote_copy(
        src_ref=src, dst_ref=dst, send_sem=send, recv_sem=recv, device_id=peer, device_id_type=MESH
    )


def spread_kernel(n_out, n_in, b_ref, q_ref, bz_ref, qf_ref, b_own, q_own, own_sem, sb, rb, sq, rq, sf, rf):
    blk, col = lax.axis_index("blk"), lax.axis_index("col")
    me_o, me_i = blk // n_in, lax.rem(blk, n_in)
    outer = [lax.rem(me_o + k, n_out) for k in range(n_out)]
    width = bz_ref.shape[-1]
    wide = [pl.ds(pl.multiple_of(o * width, LANES), width) for o in outer]
    inner = [lax.rem(me_i + k, n_in) for k in range(n_in)]
    greet(
        [(outer[k] * n_in + me_i, col) for k in range(1, n_out)]
        + [(me_o * n_in + inner[j], col) for j in range(1, n_in)]
    )
    load_b = pltpu.make_async_copy(b_ref.at[:, wide[0]], b_own, own_sem.at[0])
    load_q = pltpu.make_async_copy(q_ref.at[:, wide[0]], q_own, own_sem.at[1])
    load_b.start()
    load_q.start()
    q_sends, b_sends, forwards = [], [], []
    for k in range(1, n_out):
        peer = (outer[k] * n_in + me_i, col)
        copy = remote(q_ref.at[:, wide[k]], qf_ref.at[me_o, me_i], sq.at[k], rq.at[k], peer)
        copy.start()
        q_sends.append(copy)
    for j in range(1, n_in):
        peer = (me_o * n_in + inner[j], col)
        copy = remote(q_ref.at[:, wide[0]], qf_ref.at[me_o, me_i], sf.at[j, 0], rf.at[j, 0], peer)
        copy.start()
        forwards.append(copy)
    for k in range(1, n_out):
        peer = (outer[k] * n_in + me_i, col)
        copy = remote(b_ref.at[:, wide[k]], bz_ref.at[me_o], sb.at[k], rb.at[k], peer)
        copy.start()
        b_sends.append(copy)
    load_b.wait()
    load_q.wait()
    store_b = pltpu.make_async_copy(b_own, bz_ref.at[me_o], own_sem.at[0])
    store_q = pltpu.make_async_copy(q_own, qf_ref.at[me_o, me_i], own_sem.at[1])
    store_b.start()
    store_q.start()
    for k in range(1, n_out):
        q_sends[k - 1].wait_recv()
        came_from = lax.rem(me_o + n_out - k, n_out)
        for j in range(1, n_in):
            peer = (me_o * n_in + inner[j], col)
            piece = qf_ref.at[came_from, me_i]
            copy = remote(piece, piece, sf.at[j, k], rf.at[j, k], peer)
            copy.start()
            forwards.append(copy)
    for copy in q_sends:
        copy.wait_send()
    for copy in b_sends + forwards:
        copy.wait()
    store_b.wait()
    store_q.wait()


def spread(n_out, n_in, b_half, q_basis):
    width = b_half.shape[1] // n_out
    b_part = (b_half.shape[0], width)
    q_part = (q_basis.shape[0], width)
    any_space = pl.BlockSpec(memory_space=pl.ANY)
    dma = pltpu.SemaphoreType.DMA
    return pl.pallas_call(
        functools.partial(spread_kernel, n_out, n_in),
        out_shape=(
            jax.ShapeDtypeStruct((n_out,) + b_part, b_half.dtype),
            jax.ShapeDtypeStruct((n_out, n_in) + q_part, q_basis.dtype),
        ),
        in_specs=[any_space] * 2,
        out_specs=(any_space, any_space),
        scratch_shapes=[
            pltpu.VMEM(b_part, b_half.dtype),
            pltpu.VMEM(q_part, q_basis.dtype),
            dma((2,)),
            dma((n_out,)),
            dma((n_out,)),
            dma((n_out,)),
            dma((n_out,)),
            dma((n_in, n_out)),
            dma((n_in, n_out)),
        ],
        compiler_params=PARAMS(collective_id=0),
        name="spread",
    )(b_half, q_basis)


def left_kernel(
    n_out, n_in, n_col, n_core, rows_total, pt_ref, out_ref,
    half, summed, got, squares, squares_got, mine, s0, r0, s1, r1, s2, r2, s3, r3, s4, r4, own_sem
):
    blk, col = lax.axis_index("blk"), lax.axis_index("col")
    me_o, me_i = blk // n_in, lax.rem(blk, n_in)
    n_chip = n_col // n_core
    chip, core = col // n_core, lax.rem(col, n_core)
    members = n_out * n_chip
    me = me_o * n_chip + chip
    place, peers, source = [], [], []
    for k in range(members):
        g = lax.rem(me + k, members)
        place.append(g)
        peers.append(((g // n_chip) * n_in + me_i, lax.rem(g, n_chip) * n_core + core))
        source.append(lax.rem(me + members - k, members))
    inner_peers = [(me_o * n_in + lax.rem(me_i + j, n_in), col) for j in range(n_in)]
    cores = [lax.rem(core + j, n_core) for j in range(n_core)]
    core_peers = [(blk, chip * n_core + cores[j]) for j in range(n_core)]
    greet(peers[1:] + inner_peers[1:] + core_peers[1:])
    hand = []
    for j in range(1, n_core):
        copy = remote(pt_ref.at[cores[j]], half.at[j], s0.at[j], r0.at[j], core_peers[j])
        copy.start()
        hand.append(copy)
    for copy in hand:
        copy.wait_recv()

    def add_cores(g):
        total = pt_ref[core, g].astype(jnp.float32)
        for j in range(1, n_core):
            total = total + half[j, g].astype(jnp.float32)
        return total

    sends = []
    for k in list(range(1, members)) + [0]:
        summed[place[k]] = add_cores(place[k]).astype(summed.dtype)
        if k:
            copy = remote(summed.at[place[k]], got.at[k], s1.at[k], r1.at[k], peers[k])
            copy.start()
            sends.append(copy)
    total = add_cores(me)
    for k in range(1, members):
        sends[k - 1].wait_recv()
        total = total + got[k].astype(jnp.float32)
    square = jnp.sum(total * total, axis=1, keepdims=True)
    squares[...] = jnp.broadcast_to(square, squares.shape)
    swaps = []
    for j in range(1, n_in):
        copy = remote(squares, squares_got.at[j], s2.at[j], r2.at[j], inner_peers[j])
        copy.start()
        swaps.append(copy)
    full = squares[...]
    for j in range(1, n_in):
        swaps[j - 1].wait_recv()
        full = full + squares_got[j]
    scale = jnp.sqrt(full[:, :1] / rows_total + epsilon)
    mine[...] = (total / scale).astype(mine.dtype)
    own = pltpu.make_async_copy(mine, out_ref.at[core, me], own_sem.at[0])
    own.start()
    gathers, passes = [], []
    for k in range(1, members):
        copy = remote(mine, out_ref.at[core, me], s3.at[k], r3.at[k], peers[k])
        copy.start()
        gathers.append(copy)
    for j in range(1, n_core):
        copy = remote(mine, out_ref.at[core, me], s4.at[j, 0], r4.at[j, 0], core_peers[j])
        copy.start()
        passes.append(copy)
    for k in range(1, members):
        gathers[k - 1].wait_recv()
        for j in range(1, n_core):
            piece = out_ref.at[core, source[k]]
            copy = remote(piece, piece, s4.at[j, k], r4.at[j, k], core_peers[j])
            copy.start()
            passes.append(copy)
    for copy in hand + sends + swaps + gathers:
        copy.wait_send()
    for copy in passes:
        copy.wait()
    own.wait()


def left(n_out, n_in, n_col, rows_total, pt):
    n_core = 2 if n_col % 2 == 0 else 1
    members = n_out * n_col // n_core
    rank, rows = pt.shape
    part = rank // (members * n_core)
    dma = pltpu.SemaphoreType.DMA
    vmem = pl.BlockSpec(memory_space=pltpu.VMEM)
    shape = (n_core, members, part, rows)
    out = pl.pallas_call(
        functools.partial(left_kernel, n_out, n_in, n_col, n_core, rows_total),
        out_shape=jax.ShapeDtypeStruct(shape, pt.dtype),
        in_specs=[vmem],
        out_specs=vmem,
        scratch_shapes=[
            pltpu.VMEM(shape, pt.dtype),
            pltpu.VMEM((members, part, rows), pt.dtype),
            pltpu.VMEM((members, part, rows), pt.dtype),
            pltpu.VMEM((part, LANES), jnp.float32),
            pltpu.VMEM((n_in, part, LANES), jnp.float32),
            pltpu.VMEM((part, rows), pt.dtype),
        ]
        + [dma((n_core,))] * 2
        + [dma((members,))] * 2
        + [dma((n_in,))] * 2
        + [dma((members,))] * 2
        + [dma((n_core, members))] * 2
        + [dma((1,))],
        compiler_params=PARAMS(collective_id=1),
        name="left",
    )(pt.reshape(shape))
    return out.reshape(rank, rows)


def right_kernel(
    n_out, n_in, n_col, r_ref, full_ref, sum_ref,
    got, mine, squares, squares_got, s1, r1, sz, rz, sx, rx, s2, r2, s3, r3, own_sem
):
    blk, col = lax.axis_index("blk"), lax.axis_index("col")
    me_o, me_i = blk // n_in, lax.rem(blk, n_in)
    width = r_ref.shape[-1]
    inner = [lax.rem(me_i + j, n_in) for j in range(n_in)]
    origin = [lax.rem(me_i + n_in - j, n_in) for j in range(n_in)]
    peers = [(me_o * n_in + inner[j], col) for j in range(n_in)]
    members = n_out * n_col
    mates = []
    for k in range(members):
        g = lax.rem(me_o * n_col + col + k, members)
        mates.append(((g // n_col) * n_in + me_i, lax.rem(g, n_col)))
    greet(peers[1:] + mates[1:])
    first = list(range(n_out - n_out // 2, n_out))
    early = list(range(n_out - n_out // 2))

    def slot(p, i, o):
        return full_ref.at[p, i, :, pl.ds(pl.multiple_of(o * width, LANES), width)]

    def along(way, s, p, d, source, piece):
        peer = ((me_o + 1 if way == 0 else me_o - 1) * n_in + me_i, col)
        return remote(source, piece, sz.at[way, s, p, d], rz.at[way, s, p, d], peer)

    def can_send(way):
        return me_o < n_out - 1 if way == 0 else me_o > 0

    def came(way, d):
        return (me_o - d, me_o >= d) if way == 0 else (me_o + d, me_o + d < n_out)

    def across(j, p, index, source, piece):
        return remote(source, piece, sx.at[j, p, index], rx.at[j, p, index], peers[j])

    def mark(way, d):
        return d if way == 0 else n_out - 1 + d

    sends = {}
    for p in range(n_out):
        for j in range(1, n_in):
            copy = remote(r_ref.at[p, inner[j]], got.at[j, p], s1.at[j, p], r1.at[j, p], peers[j])
            copy.start()
            sends[j, p] = copy
    squares[...] = jnp.zeros_like(squares)
    ones = jnp.ones((8, width), jnp.float32)
    for p in range(n_out):
        for j in range(1, n_in):
            sends[j, p].wait_recv()
        total = r_ref[p, me_i].astype(jnp.float32)
        for j in range(1, n_in):
            total = total + got[j, p].astype(jnp.float32)
        mine[p] = total.astype(mine.dtype)
        squares[p] = lax.dot_general(
            ones, total * total, (((1,), (1,)), ((), ())),
            precision=lax.Precision.HIGHEST, preferred_element_type=jnp.float32,
        )
        own = slot(p, me_i, me_o)
        pltpu.make_async_copy(mine.at[p], own, own_sem.at[p]).start()
        for j in range(1, n_in):
            across(j, p, 0, mine.at[p], own).start()
        for way in range(2):
            @pl.when(can_send(way))
            def _():
                along(way, 0, p, 1, mine.at[p], own).start()
    pooled = []
    for k in range(1, members):
        copy = remote(squares, squares_got.at[k], s2.at[k], r2.at[k], mates[k])
        copy.start()
        pooled.append(copy)
    def enter(p):
        for j in range(1, n_in):
            piece = slot(p, origin[j], me_o)
            across(j, p, 0, piece, piece).wait_recv()
            for way in range(2):
                @pl.when(can_send(way))
                def _():
                    along(way, j, p, 1, piece, piece).start()

    def onward(d, p, s):
        for way in range(2):
            o, there = came(way, d)

            @pl.when(there)
            def _():
                piece = slot(p, origin[s], o)
                along(way, s, p, d, piece, piece).wait_recv()
                if d < n_out - 1:
                    @pl.when(can_send(way))
                    def _():
                        along(way, s, p, d + 1, piece, piece).start()
                if p not in first:
                    for j in range(1, n_in):
                        across(j, p, mark(way, d), piece, piece).start()

    for p in early + first:
        onward(1, p, 0)
    for p in first:
        enter(p)
    for d in range(1, n_out):
        for p in early + first:
            for s in range(n_in if p in first else 1):
                if d > 1 or s:
                    onward(d, p, s)
    total = squares[...]
    for k in range(1, members):
        pooled[k - 1].wait_recv()
        total = total + squares_got[k]
    sum_ref[0] = total
    swaps = []
    for j in range(1, n_in):
        copy = remote(sum_ref.at[0], sum_ref.at[j], s3.at[j], r3.at[j], peers[j])
        copy.start()
        swaps.append(copy)
    for p in range(n_out):
        own = slot(p, me_i, me_o)
        pltpu.make_async_copy(mine.at[p], own, own_sem.at[p]).wait()
        for j in range(1, n_in):
            across(j, p, 0, mine.at[p], own).wait_send()
            if p not in first:
                piece = slot(p, origin[j], me_o)
                across(j, p, 0, piece, piece).wait_recv()
        for s in range(n_in if p in first else 1):
            for way in range(2):
                for d in range(1, n_out):
                    o, there = came(way, d - 1)

                    @pl.when(there & can_send(way))
                    def _():
                        piece = slot(p, origin[s], o)
                        along(way, s, p, d, piece, piece).wait_send()
        if p not in first:
            for way in range(2):
                for d in range(1, n_out):
                    o, there = came(way, d)

                    @pl.when(there)
                    def _():
                        for j in range(1, n_in):
                            mark_at = mark(way, d)
                            piece = slot(p, me_i, o)
                            across(j, p, mark_at, piece, piece).wait_send()
                            piece = slot(p, origin[j], o)
                            across(j, p, mark_at, piece, piece).wait_recv()
    for copy in list(sends.values()) + pooled:
        copy.wait_send()
    for copy in swaps:
        copy.wait()


def right(n_out, n_in, n_col, r):
    rank, width = r.shape
    part = rank // (n_out * n_in)
    members = n_out * n_col
    dma = pltpu.SemaphoreType.DMA
    vmem = pl.BlockSpec(memory_space=pltpu.VMEM)
    full, sums = pl.pallas_call(
        functools.partial(right_kernel, n_out, n_in, n_col),
        out_shape=(
            jax.ShapeDtypeStruct((n_out, n_in, part, n_out * width), r.dtype),
            jax.ShapeDtypeStruct((n_in, n_out, 8, part), jnp.float32),
        ),
        in_specs=[vmem],
        out_specs=(pl.BlockSpec(memory_space=pl.ANY), vmem),
        scratch_shapes=[
            pltpu.VMEM((n_in, n_out, part, width), r.dtype),
            pltpu.VMEM((n_out, part, width), r.dtype),
            pltpu.VMEM((n_out, 8, part), jnp.float32),
            pltpu.VMEM((members, n_out, 8, part), jnp.float32),
        ]
        + [dma((n_in, n_out))] * 2
        + [dma((2, n_in, n_out, n_out))] * 2
        + [dma((n_in, n_out, 2 * n_out - 1))] * 2
        + [dma((members,))] * 2
        + [dma((n_in,))] * 2
        + [dma((n_out,))],
        compiler_params=PARAMS(collective_id=2),
        name="right",
    )(r.reshape(n_out, n_in, part, width))
    me_i = lax.rem(lax.axis_index("blk"), n_in)
    order = lax.rem(me_i - jnp.arange(n_in) + n_in, n_in)
    sums = jnp.take(sums[:, :, 0, :], order, axis=0).transpose(1, 0, 2).reshape(rank)
    return full.reshape(rank, n_out * width), sums


def shards(n_blk, n_col, momentum, grad, q_basis):
    n_out = 4 if n_blk % 4 == 0 else n_blk
    n_in = n_blk // n_out
    rows, cols = momentum.shape
    rank_rows = q_basis.shape[0]
    rank = rank_rows * n_blk
    rows_total, feature_count = rows * n_blk, cols * n_col
    width = -(-cols // (n_out * LANES)) * LANES
    pad = ((0, 0), (0, n_out * width - cols))

    b_matrix = momentum + grad.astype(jnp.float32)
    bz, qf = spread(n_out, n_in, jnp.pad(b_matrix.astype(jnp.bfloat16), pad), jnp.pad(q_basis, pad))
    bz = bz.reshape(n_out * rows, width)
    qf = qf.reshape(rank, width)
    pt = lax.dot_general(qf, bz, (((1,), (1,)), ((), ())), preferred_element_type=jnp.float32)
    p_hat_t = left(n_out, n_in, n_col, rows_total, pt.astype(jnp.bfloat16))
    r_part = jnp.dot(p_hat_t, bz, preferred_element_type=jnp.float32).astype(jnp.bfloat16)
    r_sum, squares = right(n_out, n_in, n_col, r_part)
    r_scale = jnp.sqrt(squares / feature_count + epsilon)
    blk = lax.axis_index("blk")
    p_mine = lax.dynamic_slice_in_dim(p_hat_t, (blk // n_in) * rows, rows, 1)
    p_even = (p_mine.astype(jnp.float32) / r_scale[:, None]).astype(jnp.bfloat16)
    over = (((0,), (0,)), ((), ()))
    correction = lax.dot_general(p_mine, r_sum, over, preferred_element_type=jnp.float32)[:, :cols]
    update = lax.dot_general(p_even, r_sum, over, preferred_element_type=jnp.float32)[:, :cols]
    update = (update * (1.0 / jnp.sqrt(jnp.float32(rank)))).astype(jnp.bfloat16)
    start = blk * rank_rows
    r_mine = lax.dynamic_slice_in_dim(r_sum, start, rank_rows, 0)[:, :cols].astype(jnp.float32)
    scale_mine = lax.dynamic_slice_in_dim(r_scale, start, rank_rows, 0)
    q_new = (r_mine / scale_mine[:, None]).astype(jnp.bfloat16)
    return (b_matrix - correction * (decay_rest / rows_total), update, q_new)


def solution(mesh):
    in_specs = (P("blk", "col"), P("blk", "col"), P("blk", "col"))
    out_specs = (P("blk", "col"), P("blk", "col"), P("blk", "col"))
    body = functools.partial(shards, mesh.shape["blk"], mesh.shape["col"])
    return jax.shard_map(body, mesh=mesh, in_specs=in_specs, out_specs=out_specs, check_vma=False)
```
